32 devices in a mesh: dp: 4 (over y, x), shard: 8 (over z, core).
Axes of the slice: x: 2, y: 2, z: 4, core: 2. Of those that a mesh axis runs over, the one named last changes fastest.
Arguments:
- gradients: bfloat16 [4, 4, 786432], P('dp', None, 'shard'), may hold values from -32 to 32
- master: float32 [3145728], P(('dp', 'shard'))
- moment: float32 [3145728], P(('dp', 'shard')), may hold values from -1.5 to 1.5
- second: float32 [3145728], P(('dp', 'shard')), may hold values from 0.05 to 2
- segment_ids: int32 [24576], P(('dp', 'shard')), may hold values from 0 to 15, never falling along the last dimension, each value on 1 to 3072 neighbouring positions
Outputs:
- weights: bfloat16 [4, 786432], P(None, 'shard')
- new_master: float32 [3145728], P(('dp', 'shard'))
- new_moment: float32 [3145728], P(('dp', 'shard'))
- new_second: float32 [3145728], P(('dp', 'shard'))
The draws below stay inside these ranges and needn't reach their ends.
Inputs may be any that keep to these rules, and one draw needn't show every extreme that they name: segment_ids never falls along the flat vector; each tensor has 1 to 3072 blocks and one has exactly 3072.
All inputs are finite; a program needn't handle non-finite values.
Results may differ from the reference program's by a relative error of at most 0.0004.
Values may be sent and summed in bfloat16 or wider, within the bound.
No kernel may reach another device: no remote copies, remote signals or barrier semaphores. Data moves between devices by JAX's collectives and lax.ppermute only.
A program may use at most 64 MiB of HBM per device.

```python
import math
import jax
import jax.numpy as jnp
import numpy as np
from jax import lax

BLOCK = 128
LOCAL_BLOCKS = 768
FLAT = 3145728
TENSORS = 16
MOST = 3072
N_DP = 4
DEVICES = 32


def draw_master(key, part):
    noise_key = jax.random.fold_in(key, 11)
    scale_key = jax.random.fold_in(key, 12)
    range_key = jax.random.fold_in(key, 13)
    position = jnp.arange(FLAT, dtype=jnp.float32) / FLAT
    rising = jnp.exp(jnp.log(3.0) * position)
    block_scale = jax.random.uniform(scale_key, (FLAT // BLOCK,), jnp.float32, 0.5, 2.0)
    block_scale = jnp.repeat(block_scale, BLOCK)
    ranges = FLAT // (BLOCK * LOCAL_BLOCKS)
    range_log = jax.random.uniform(range_key, (ranges,), jnp.float32, 0.0, jnp.log(10.0))
    range_scale = jnp.repeat(jnp.exp(range_log), BLOCK * LOCAL_BLOCKS)
    values = jax.random.normal(noise_key, (FLAT,), jnp.float32)
    values = values * rising * block_scale * range_scale
    return values.astype(jnp.float32)


def raised(array, rng, source, target, parts, factor):
    def block_of(dim):
        return (jnp.arange(array.shape[dim]) // (array.shape[dim] // parts)).reshape((-1,) + (1,) * (array.ndim - 1 - dim))

    near = jax.random.permutation(rng, parts)[block_of(target)]
    far = (block_of(target) + parts // 2) % parts
    return jnp.where((block_of(source) == near) | (block_of(source) == far), factor * array, array)


def shard_levels(rng, dims, cuts, least, top_value):
    level, own = 1.0, jax.random.fold_in(rng, 6)
    for axis_at, parts in cuts:
        draws = jnp.exp(jax.random.uniform(jax.random.fold_in(own, axis_at), (parts,), jnp.float32, least / len(cuts), top_value / len(cuts)))
        level = level * jnp.repeat(draws, dims[axis_at] // parts).reshape([-1 if axis == axis_at else 1 for axis in range(len(dims))])
    return level


def split_up(count, total, bound, slope):
    portions = [(1 << 20) // math.isqrt(rank ** slope) + 1 for rank in range(2, count + 1)]
    surplus, counts = total - bound - (count - 1), [1] * (count - 1)
    while surplus > 0:
        free = [i for i in range(count - 1) if counts[i] < bound]
        whole, remaining = sum([portions[i] for i in free]), surplus
        for i in free:
            addition = min(bound - counts[i], max(1, remaining * portions[i] // whole), surplus)
            counts[i] = counts[i] + addition
            surplus = surplus - addition
    return np.array([bound] + counts)


def uneven(stream_key, number_of, total, bound, lean):
    if number_of == 2:
        one = jax.random.randint(stream_key, (), max(1, total - bound), min(bound, total - 1) + 1)
        return jnp.stack([one, total - one])
    lengths = jnp.asarray(split_up(number_of, total, bound, lean), jnp.int32)
    couples = (number_of - 1) // 2
    source_of, taker = lengths[1:1 + 2 * couples:2], lengths[2:2 + 2 * couples:2]
    margin = jnp.minimum(source_of - 1, bound - taker)
    moved = jax.random.randint(jax.random.fold_in(stream_key, 1), (couples,), 0, 1 << 20) % (margin + 1)
    lengths = lengths.at[1:1 + 2 * couples:2].set(source_of - moved).at[2:2 + 2 * couples:2].set(taker + moved)
    return lengths[jax.random.permutation(jax.random.fold_in(stream_key, 2), number_of)]


def normal_values(rng, extent, width, limit, pieces=(), kind=jnp.bfloat16):
    drawn = width * jax.random.normal(rng, extent, jnp.float32)
    if pieces:
        drawn = drawn * shard_levels(rng, extent, pieces, -0.22, 0.18)
    return jnp.clip(drawn, -limit, limit).astype(kind)


def gaussian_with(stream_key, dims, spread, limit, pieces, heavy, kind=jnp.bfloat16):
    result = spread * jax.random.normal(stream_key, dims, jnp.float32)
    if pieces:
        result = result * shard_levels(stream_key, dims, pieces, -0.22, 0.18)
    return jnp.clip(raised(result, jax.random.fold_in(stream_key, 3), *heavy), -limit, limit).astype(kind)


def setup_inputs(seed: int = 0) -> dict:
    key_list = jax.random.split(jax.random.key(seed), 6)
    gradients = gaussian_with(key_list[0], (N_DP, N_DP, FLAT // N_DP), 4.0, 32.0, ((0, 4), (2, 8)), (0, 1, 4, 2.0))
    master = draw_master(jax.random.fold_in(key_list[5], 71), 0)
    moment = normal_values(key_list[2], (FLAT,), 0.1, 1.5, ((0, 32),), jnp.float32)
    second = jnp.clip(jnp.exp(math.log(2.0) - 3.6888794 * jax.random.uniform(key_list[3], (FLAT,), jnp.float32) ** shard_levels(key_list[3], (FLAT,), ((0, 32),), -0.2, 0.2)), 0.05, 2.0)
    segment_ids = jnp.searchsorted(jnp.cumsum(uneven(key_list[4], TENSORS, LOCAL_BLOCKS * DEVICES, MOST, 2)), jnp.arange(LOCAL_BLOCKS * DEVICES), side="right").astype(jnp.int32)
    return {"gradients": gradients, "master": master, "moment": moment, "second": second, "segment_ids": segment_ids}


first_fix = 1.0 - 0.9 ** 20
second_fix = 1.0 - 0.999 ** 20
learn_rate = 0.2
decay_rate = 0.01
tiny_eps = 1e-06

def reference(gradients, master, moment, second, segment_ids):
    grad = lax.optimization_barrier(jnp.sum(gradients.astype(jnp.float32), axis=0)).reshape(-1) / N_DP
    new_moment = 0.9 * moment + 0.1 * grad
    new_second = 0.999 * second + 0.001 * grad * grad
    update = new_moment / first_fix / (jnp.sqrt(new_second / second_fix) + tiny_eps) + decay_rate * master
    weight_blocks = lax.optimization_barrier(jnp.sum((master * master).reshape(-1, BLOCK), axis=1))
    update_blocks = lax.optimization_barrier(jnp.sum((update * update).reshape(-1, BLOCK), axis=1))
    weight_sq = jax.ops.segment_sum(weight_blocks, segment_ids, num_segments=TENSORS)
    update_sq = jax.ops.segment_sum(update_blocks, segment_ids, num_segments=TENSORS)
    trust = jnp.sqrt(weight_sq) / (jnp.sqrt(update_sq) + tiny_eps)
    block_trust = trust[segment_ids]
    new_master = master - learn_rate * (update.reshape(-1, BLOCK) * block_trust[:, None]).reshape(-1)
    weights = new_master.astype(jnp.bfloat16).reshape(N_DP, -1)
    return (weights, new_master, new_moment, new_second)
```

```python
import jax
import jax.numpy as jnp
from jax import lax
from jax.sharding import PartitionSpec as P

first_fix = 1.0 - 0.9**20
second_fix = 1.0 - 0.999**20
learn_rate = 0.2
decay_rate = 0.01
tiny_eps = 1e-06
both = ("dp", "shard")


def swap(value, step, count):
    return lax.ppermute(value, "dp", [(i, i ^ step) for i in range(count)])


def moments(summed, master_part, moment_part, second_part, replicas):
    grad = summed / replicas
    next_moment = 0.9 * moment_part + 0.1 * grad
    next_second = 0.999 * second_part + 0.001 * grad * grad
    update_dir = (
        next_moment / first_fix / (jnp.sqrt(next_second / second_fix) + tiny_eps)
        + decay_rate * master_part
    )
    return (next_moment, next_second, update_dir)


def tensor_sums(values, onehot):
    block_sq = jnp.sum((values * values).reshape(onehot.shape[0], -1), axis=1)
    return jnp.dot(block_sq, onehot, precision=lax.Precision.HIGHEST)


def on_device(gradients, master, moment, second, segment_ids):
    replicas = lax.axis_size("dp")
    devices = replicas * lax.axis_size("shard")
    tensors = devices // 2
    blocks = segment_ids.shape[0]
    mine = lax.axis_index("dp")
    onehot = (segment_ids[:, None] == jnp.arange(tensors, dtype=jnp.int32)[None, :]).astype(
        jnp.float32
    )
    rows = [
        lax.dynamic_index_in_dim(gradients[0], mine ^ k, 0, keepdims=False) for k in range(replicas)
    ]
    received = {k: swap(rows[k], k, replicas) for k in reversed(range(1, replicas))}
    summed = rows[0].astype(jnp.float32)
    for k in range(1, replicas):
        summed = summed + received[k].astype(jnp.float32)
    new_moment, new_second, update_dir = moments(summed, master, moment, second, replicas)
    sums = jnp.concatenate([tensor_sums(master, onehot), tensor_sums(update_dir, onehot)])
    spread = jnp.broadcast_to(sums[None, :], (devices, 2 * tensors))
    totals = jnp.sum(lax.all_to_all(spread, both, 0, 0, tiled=True), axis=0)
    trust = jnp.sqrt(totals[:tensors]) / (jnp.sqrt(totals[tensors:]) + tiny_eps)
    block_trust = jnp.dot(onehot, trust, precision=lax.Precision.HIGHEST)
    new_master = master - learn_rate * (
        update_dir.reshape(blocks, -1) * block_trust[:, None]
    ).reshape(-1)
    rounded = new_master.astype(jnp.bfloat16)
    weights = lax.all_gather(rounded[None, :], "dp", axis=0, tiled=True)
    return (weights, new_master, new_moment, new_second)


def solution(mesh):
    placed = (
        P("dp", None, "shard"),
        P(("dp", "shard")),
        P(("dp", "shard")),
        P(("dp", "shard")),
        P(("dp", "shard")),
    )
    return jax.shard_map(
        on_device,
        mesh=mesh,
        in_specs=placed,
        out_specs=(P(None, "shard"), P(("dp", "shard")), P(("dp", "shard")), P(("dp", "shard"))),
        check_vma=False,
    )
```

```python
import functools

import jax
import jax.numpy as jnp
from jax import lax
from jax.experimental import pallas as pl
from jax.experimental.pallas import tpu as pltpu
from jax.sharding import PartitionSpec as P

first_fix = 1.0 - 0.9**20
second_fix = 1.0 - 0.999**20
learn_rate = 0.2
decay_rate = 0.01
tiny_eps = 1e-06
both = ("dp", "shard")
lanes = 128
f32, bf16 = jnp.float32, jnp.bfloat16
grant = 8 << 20
exact = functools.partial(
    lax.dot_general, precision=lax.Precision.HIGHEST, preferred_element_type=f32
)


def call(kernel, outs, scratch=(), work=1 << 20):
    return pl.pallas_call(
        kernel,
        out_shape=outs,
        scratch_shapes=list(scratch),
        compiler_params=pltpu.CompilerParams(vmem_limit_bytes=grant),
        cost_estimate=pl.CostEstimate(flops=work, bytes_accessed=work, transcendentals=0),
    )


def split_kernel(step, group, gradients, *rest):
    rows, room = rest[:-1], rest[-1]
    count = len(rows)
    mine = lax.axis_index("dp")

    def body(j, _):
        for at in range(0, step, group):
            start = pl.multiple_of((j * step + at) * lanes, group * lanes)
            wide = gradients[:, pl.ds(start, group * lanes)].astype(f32)
            for t in range(group):
                room[(at + t) * count : (at + t + 1) * count, :] = wide[
                    :, t * lanes : (t + 1) * lanes
                ]
        for k in range(count):
            rows[k][pl.ds(pl.multiple_of(j * step, step), step), :] = room[
                pl.ds(mine ^ k, step, stride=count), :
            ].astype(bf16)
        return 0

    lax.fori_loop(0, gradients.shape[1] // lanes // step, body, 0)


def chosen(ids, start, step, tensors):
    return (
        ids[:, pl.ds(start, step)] == lax.broadcasted_iota(jnp.int32, (tensors, step), 0)
    ).astype(f32)


def moments_kernel(step, tensors, replicas, ids, master, moment, second, *rest):
    rows = rest[:replicas]
    new_moment, new_second, update_dir, spread = rest[replicas:]

    def body(j, sums):
        start = pl.multiple_of(j * step, step)
        part = pl.ds(start, step)
        summed = rows[0][part, :].astype(f32)
        for row in rows[1:]:
            summed = summed + row[part, :].astype(f32)
        grad = summed / replicas
        old = master[part, :]
        first = 0.9 * moment[part, :] + 0.1 * grad
        squared = 0.999 * second[part, :] + 0.001 * grad * grad
        step_dir = first * (1.0 / first_fix) / (
            jnp.sqrt(squared * (1.0 / second_fix)) + tiny_eps
        ) + decay_rate * old
        new_moment[part, :] = first
        new_second[part, :] = squared
        update_dir[part, :] = step_dir
        hot = chosen(ids, start, step, tensors)
        both_sq = jnp.concatenate([old * old, step_dir * step_dir], axis=1)
        return sums + exact(hot, both_sq, (((1,), (0,)), ((), ())))

    sums = lax.fori_loop(
        0, master.shape[0] // step, body, jnp.zeros((tensors, 2 * lanes), f32)
    )
    stacked = jnp.concatenate([sums[:, :lanes], sums[:, lanes:]], axis=0)
    line = exact(jnp.ones((8, lanes), f32), stacked, (((1,), (1,)), ((), ())))
    spread[...] = jnp.broadcast_to(line[:1][None], spread.shape)


def apply_kernel(step, tensors, gathered, ids, master, update_dir, rounded, new_master):
    devices = gathered.shape[0]
    parts = gathered[...].reshape(devices, 2 * tensors)
    totals = exact(parts, jnp.ones((devices, lanes), f32), (((0,), (0,)), ((), ())))
    trust = jnp.sqrt(totals[:tensors]) / (jnp.sqrt(totals[tensors:]) + tiny_eps)

    def body(j, _):
        start = pl.multiple_of(j * step, step)
        part = pl.ds(start, step)
        hot = chosen(ids, start, step, tensors)
        scale = exact(hot, trust, (((0,), (0,)), ((), ())))
        fresh = master[part, :] - learn_rate * (update_dir[part, :] * scale)
        new_master[part, :] = fresh
        rounded[part, :] = fresh.astype(bf16)
        return 0

    lax.fori_loop(0, master.shape[0] // step, body, 0)


def join_kernel(step, group, rows, weights, room):
    count = weights.shape[0]
    blocks = rows.shape[0] // count

    def body(j, _):
        for k in range(count):
            room[pl.ds(k, step, stride=count), :] = rows[
                pl.ds(pl.multiple_of(k * blocks + j * step, step), step), :
            ].astype(f32)
        for at in range(step):
            start = pl.multiple_of((j * step + at) * lanes, lanes)
            weights[:, pl.ds(start, lanes)] = room[at * count : (at + 1) * count, :].astype(bf16)
        return 0

    lax.fori_loop(0, blocks // step, body, 0)


def on_device(gradients, master, moment, second, segment_ids):
    replicas = lax.axis_size("dp")
    devices = replicas * lax.axis_size("shard")
    tensors = devices // 2
    blocks = segment_ids.shape[0]
    ids = segment_ids.reshape(1, blocks)
    master, moment, second = (a.reshape(blocks, lanes) for a in (master, moment, second))
    row = jax.ShapeDtypeStruct((blocks, lanes), bf16)
    wide = jax.ShapeDtypeStruct((blocks, lanes), f32)
    step = 128

    rows = call(
        functools.partial(split_kernel, step, 8),
        [row] * replicas,
        [pltpu.VMEM((step * replicas, lanes), f32)],
    )(gradients[0])
    received = {
        k: lax.ppermute(rows[k], "dp", [(i, i ^ k) for i in range(replicas)])
        for k in reversed(range(1, replicas))
    }
    new_moment, new_second, update_dir, spread = call(
        functools.partial(moments_kernel, step, tensors, replicas),
        [wide, wide, wide, jax.ShapeDtypeStruct((devices, 1, 2 * tensors), f32)],
    )(ids, master, moment, second, rows[0], *(received[k] for k in range(1, replicas)))
    gathered = lax.all_to_all(spread, both, 0, 0, tiled=True)
    rounded, new_master = call(
        functools.partial(apply_kernel, step, tensors), [row, wide]
    )(gathered, ids, master, update_dir)
    whole = lax.all_gather(rounded, "dp", axis=0, tiled=True)
    weights = call(
        functools.partial(join_kernel, step, 8),
        jax.ShapeDtypeStruct((replicas, blocks * lanes), bf16),
        [pltpu.VMEM((step * replicas, lanes), f32)],
    )(whole)
    return (weights, new_master.reshape(-1), new_moment.reshape(-1), new_second.reshape(-1))


def solution(mesh):
    placed = (
        P("dp", None, "shard"),
        P(("dp", "shard")),
        P(("dp", "shard")),
        P(("dp", "shard")),
        P(("dp", "shard")),
    )
    return jax.shard_map(
        on_device,
        mesh=mesh,
        in_specs=placed,
        out_specs=(P(None, "shard"), P(("dp", "shard")), P(("dp", "shard")), P(("dp", "shard"))),
        check_vma=False,
    )
```

```python
import functools

import jax
import jax.numpy as jnp
from jax import lax
from jax.experimental import pallas as pl
from jax.experimental.pallas import tpu as pltpu
from jax.sharding import PartitionSpec as P

first_fix = 1.0 - 0.9**20
second_fix = 1.0 - 0.999**20
learn_rate = 0.2
decay_rate = 0.01
tiny_eps = 1e-06
both = ("dp", "shard")
lanes = 128
pieces = 6
f32, bf16 = jnp.float32, jnp.bfloat16
grant = 8 << 20


def call(kernel, outs, scratch=(), work=1 << 20, **specs):
    return pl.pallas_call(
        kernel,
        out_shape=outs,
        scratch_shapes=list(scratch),
        compiler_params=pltpu.CompilerParams(vmem_limit_bytes=grant),
        cost_estimate=pl.CostEstimate(flops=work, bytes_accessed=work, transcendentals=0),
        **specs,
    )


def halves(value):
    high = value.astype(bf16)
    return high, (value - high.astype(f32)).astype(bf16)


def thirds(value):
    high, rest = value.astype(bf16), value
    rest = value - high.astype(f32)
    middle = rest.astype(bf16)
    return high, middle, (rest - middle.astype(f32)).astype(bf16)


def split_kernel(step, group, gradients, *rest):
    rows, room = rest[:-1], rest[-1]
    count = len(rows)
    mine = lax.axis_index("dp")

    def body(j, _):
        for at in range(0, step, group):
            start = pl.multiple_of((j * step + at) * lanes, group * lanes)
            wide = gradients[:, pl.ds(start, group * lanes)].astype(f32)
            for t in range(group):
                room[(at + t) * count : (at + t + 1) * count, :] = wide[
                    :, t * lanes : (t + 1) * lanes
                ]
        for k in range(count):
            rows[k][pl.ds(pl.multiple_of(j * step, step), step), :] = room[
                pl.ds(mine ^ k, step, stride=count), :
            ].astype(bf16)
        return 0

    lax.fori_loop(0, gradients.shape[1] // lanes // step, body, 0)


def join_kernel(step, rows, new_master, weights, room, buffer, sems):
    count = weights.shape[0]
    blocks = rows.shape[0] // count
    width = weights.shape[1] // pieces
    copies = [
        pltpu.make_async_copy(
            buffer.at[:, pl.ds(p * width, width)], weights.at[:, pl.ds(p * width, width)], sems.at[p]
        )
        for p in range(pieces)
    ]

    def body(j, _):
        for k in range(count):
            room[pl.ds(k, step, stride=count), :] = rows[
                pl.ds(pl.multiple_of(k * blocks + j * step, step), step), :
            ].astype(f32)
        for at in range(step):
            start = pl.multiple_of((j * step + at) * lanes, lanes)
            buffer[:, pl.ds(start, lanes)] = room[at * count : (at + 1) * count, :].astype(bf16)
        return 0

    turns = width // lanes // step
    for p, copy in enumerate(copies):
        lax.fori_loop(p * turns, (p + 1) * turns, body, 0)
        copy.start()
    for copy in copies:
        copy.wait()


def prepare_kernel(tensors, ids, master, moment, second, old_moment, old_second, by_tensor, by_block, sums):
    blocks = ids.shape[1]
    thrice = by_block.shape[1]
    total = jnp.zeros((tensors, 2 * lanes), f32)
    for start in range(0, blocks, lanes):
        part = slice(start, start + lanes)
        old_moment[part, :] = 0.9 * moment[part, :]
        old_second[part, :] = 0.999 * second[part, :]
        tensor = lax.broadcasted_iota(jnp.int32, (thrice, lanes), 0)
        wrapped = sum(
            jnp.where((tensor >= k * tensors) & (tensor < (k + 1) * tensors), tensor - k * tensors, 0)
            for k in range(3)
        )
        inside = tensor < 3 * tensors
        hot = jnp.where(inside & (ids[:, part] == wrapped), 1.0, 0.0)
        by_tensor[:, part] = hot[:tensors].astype(bf16)
        for at in range(0, thrice, lanes):
            by_block[part, at : at + lanes] = hot[at : at + lanes].T.astype(bf16)
        old = master[part, :]
        total = total + jnp.dot(
            hot[:tensors].astype(bf16),
            jnp.concatenate(halves(old * old), axis=1),
            preferred_element_type=f32,
        )
    sums[...] = as_line(total, tensors, 0)


def as_line(total, tensors, first):
    column = jnp.sum(total[:, :lanes] + total[:, lanes:], axis=1, keepdims=True)
    shape = (tensors, 2 * tensors)
    here = (
        lax.broadcasted_iota(jnp.int32, shape, 1) == lax.broadcasted_iota(jnp.int32, shape, 0) + first
    )
    return jnp.sum(jnp.where(here, jnp.broadcast_to(column, shape), 0.0), axis=0, keepdims=True)


def direction(new_moment, new_second, master):
    return new_moment * (1.0 / first_fix) / (
        jnp.sqrt(new_second * (1.0 / second_fix)) + tiny_eps
    ) + decay_rate * master


def sums_kernel(tensors, by_tensor, master, new_moment, new_second, weight_line, spread):
    total = jnp.zeros((tensors, 2 * lanes), f32)
    for start in range(0, by_tensor.shape[1], 2 * lanes):
        part = slice(start, start + 2 * lanes)
        update_dir = direction(new_moment[part, :], new_second[part, :], master[part, :])
        total = total + jnp.dot(
            by_tensor[:, part],
            jnp.concatenate(halves(update_dir * update_dir), axis=1),
            preferred_element_type=f32,
        )
    line = weight_line[...] + as_line(total, tensors, tensors)
    spread[...] = jnp.broadcast_to(line[None], spread.shape)


def apply_kernel(tensors, gathered, by_block, master, new_moment, new_second, change):
    line = jnp.sum(gathered[...], axis=0)
    trust = jnp.sqrt(line[:, :tensors]) / (jnp.sqrt(line[:, tensors:]) + tiny_eps)
    square = (tensors, tensors)
    here = lax.broadcasted_iota(jnp.int32, square, 1) == lax.broadcasted_iota(jnp.int32, square, 0)
    column = jnp.sum(jnp.where(here, jnp.broadcast_to(trust, square), 0.0), axis=1, keepdims=True)
    parts = list(thirds(jnp.broadcast_to(column, (tensors, lanes))))
    thrice = by_block.shape[1]
    if thrice > 3 * tensors:
        parts.append(jnp.zeros((thrice - 3 * tensors, lanes), bf16))
    parts = jnp.concatenate(parts, axis=0)
    for start in range(0, master.shape[0], lanes):
        part = slice(start, start + lanes)
        scale = jnp.dot(by_block[part, :], parts, preferred_element_type=f32)
        update_dir = direction(new_moment[part, :], new_second[part, :], master[part, :])
        change[part, :] = learn_rate * (update_dir * scale)


def on_device(gradients, master, moment, second, segment_ids):
    replicas = lax.axis_size("dp")
    devices = replicas * lax.axis_size("shard")
    tensors = devices // 2
    blocks = segment_ids.shape[0]
    thrice = pl.cdiv(3 * tensors, lanes) * lanes
    ids = segment_ids.reshape(1, blocks)
    master, moment, second = (a.reshape(blocks, lanes) for a in (master, moment, second))
    row = jax.ShapeDtypeStruct((blocks, lanes), bf16)
    wide = jax.ShapeDtypeStruct((blocks, lanes), f32)
    step = 128
    far = pl.BlockSpec(memory_space=pltpu.HBM)
    near = pl.BlockSpec(memory_space=pltpu.VMEM)
    layout = (replicas, blocks * lanes)
    scratch = [
        pltpu.VMEM((step * replicas, lanes), f32),
        pltpu.VMEM(layout, bf16),
        pltpu.SemaphoreType.DMA((pieces,)),
    ]

    rows = call(
        functools.partial(split_kernel, step, 8), [row] * replicas, scratch[:1]
    )(gradients[0])
    received = {
        k: lax.ppermute(rows[k], "dp", [(i, i ^ k) for i in range(replicas)])
        for k in reversed(range(1, replicas))
    }
    old_moment, old_second, by_tensor, by_block, weight_line = call(
        functools.partial(prepare_kernel, tensors),
        [
            wide,
            wide,
            jax.ShapeDtypeStruct((tensors, blocks), bf16),
            jax.ShapeDtypeStruct((blocks, thrice), bf16),
            jax.ShapeDtypeStruct((1, 2 * tensors), f32),
        ],
    )(ids, master, moment, second)
    summed = rows[0].astype(f32)
    for k in range(1, replicas):
        summed = summed + received[k].astype(f32)
    grad = summed / replicas
    new_moment = old_moment + 0.1 * grad
    new_second = old_second + 0.001 * grad * grad
    spread = call(
        functools.partial(sums_kernel, tensors),
        jax.ShapeDtypeStruct((devices, 1, 2 * tensors), f32),
    )(by_tensor, master, new_moment, new_second, weight_line)
    gathered = lax.all_to_all(spread, both, 0, 0, tiled=True)
    change = call(functools.partial(apply_kernel, tensors), wide)(
        gathered, by_block, master, new_moment, new_second
    )
    new_master = master - change
    whole = lax.all_gather(new_master.astype(bf16), "dp", axis=0, tiled=True)
    weights = call(
        functools.partial(join_kernel, step),
        jax.ShapeDtypeStruct(layout, bf16),
        scratch,
        in_specs=[near, near],
        out_specs=far,
    )(whole, new_master)
    return (weights, new_master.reshape(-1), new_moment.reshape(-1), new_second.reshape(-1))


def solution(mesh):
    placed = (
        P("dp", None, "shard"),
        P(("dp", "shard")),
        P(("dp", "shard")),
        P(("dp", "shard")),
        P(("dp", "shard")),
    )
    return jax.shard_map(
        on_device,
        mesh=mesh,
        in_specs=placed,
        out_specs=(P(None, "shard"), P(("dp", "shard")), P(("dp", "shard")), P(("dp", "shard"))),
        check_vma=False,
    )
```

```python
import functools

import jax
import jax.numpy as jnp
from jax import lax
from jax.experimental import pallas as pl
from jax.experimental.pallas import tpu as pltpu
from jax.sharding import PartitionSpec as P

first_fix = 1.0 - 0.9**20
second_fix = 1.0 - 0.999**20
learn_rate = 0.2
decay_rate = 0.01
tiny_eps = 1e-06
both = ("dp", "shard")
lanes = 128
pieces = 6
f32, bf16 = jnp.float32, jnp.bfloat16
grant = 8 << 20


def call(kernel, outs, scratch=(), work=1 << 20, **specs):
    return pl.pallas_call(
        kernel,
        out_shape=outs,
        scratch_shapes=list(scratch),
        compiler_params=pltpu.CompilerParams(vmem_limit_bytes=grant),
        cost_estimate=pl.CostEstimate(flops=work, bytes_accessed=work, transcendentals=0),
        **specs,
    )


def halves(value):
    high = value.astype(bf16)
    return high, (value - high.astype(f32)).astype(bf16)


def thirds(value):
    high, rest = value.astype(bf16), value
    rest = value - high.astype(f32)
    middle = rest.astype(bf16)
    return high, middle, (rest - middle.astype(f32)).astype(bf16)


def split_kernel(step, gradients, *rest):
    rows, room = rest[:-1], rest[-1]
    count = len(rows)
    mine = lax.axis_index("dp")

    def body(j, _):
        part = pl.ds(pl.multiple_of(j * step, step), step)
        room[...] = gradients[:, pl.ds(pl.multiple_of(j * step * lanes, lanes), step * lanes)].astype(f32)
        for k in range(count):
            rows[k][part, :] = room[pl.ds(mine ^ k, 1), :].reshape(step, lanes).astype(bf16)
        return 0

    lax.fori_loop(0, gradients.shape[1] // lanes // step, body, 0)


def join_kernel(step, rows, new_master, weights, room, buffer, sems):
    count = weights.shape[0]
    blocks = rows.shape[0] // count
    width = weights.shape[1] // pieces
    copies = [
        pltpu.make_async_copy(
            buffer.at[:, pl.ds(p * width, width)], weights.at[:, pl.ds(p * width, width)], sems.at[p]
        )
        for p in range(pieces)
    ]

    def body(j, _):
        for k in range(count):
            room[k : k + 1, :] = (
                rows[pl.ds(pl.multiple_of(k * blocks + j * step, step), step), :]
                .astype(f32)
                .reshape(1, step * lanes)
            )
        start = pl.multiple_of(j * step * lanes, lanes)
        buffer[:, pl.ds(start, step * lanes)] = room[...].astype(bf16)
        return 0

    turns = width // lanes // step
    for p, copy in enumerate(copies):
        lax.fori_loop(p * turns, (p + 1) * turns, body, 0)
        copy.start()
    for copy in copies:
        copy.wait()


def prepare_kernel(tensors, ids, master, moment, second, old_moment, old_second, by_tensor, by_block, sums):
    blocks = ids.shape[1]
    thrice = by_block.shape[1]
    total = jnp.zeros((tensors, 2 * lanes), f32)
    for start in range(0, blocks, lanes):
        part = slice(start, start + lanes)
        old_moment[part, :] = 0.9 * moment[part, :]
        old_second[part, :] = 0.999 * second[part, :]
        tensor = lax.broadcasted_iota(jnp.int32, (thrice, lanes), 0)
        wrapped = sum(
            jnp.where((tensor >= k * tensors) & (tensor < (k + 1) * tensors), tensor - k * tensors, 0)
            for k in range(3)
        )
        inside = tensor < 3 * tensors
        hot = jnp.where(inside & (ids[:, part] == wrapped), 1.0, 0.0)
        by_tensor[:, part] = hot[:tensors].astype(bf16)
        for at in range(0, thrice, lanes):
            by_block[part, at : at + lanes] = hot[at : at + lanes].T.astype(bf16)
        old = master[part, :]
        total = total + jnp.dot(
            hot[:tensors].astype(bf16),
            jnp.concatenate(halves(old * old), axis=1),
            preferred_element_type=f32,
        )
    sums[...] = as_line(total, tensors, 0)


def as_line(total, tensors, first):
    column = jnp.sum(total[:, :lanes] + total[:, lanes:], axis=1, keepdims=True)
    shape = (tensors, 2 * tensors)
    here = (
        lax.broadcasted_iota(jnp.int32, shape, 1) == lax.broadcasted_iota(jnp.int32, shape, 0) + first
    )
    return jnp.sum(jnp.where(here, jnp.broadcast_to(column, shape), 0.0), axis=0, keepdims=True)


def direction(new_moment, new_second, master):
    fixed = new_second * (1.0 / second_fix)
    return new_moment * (1.0 / first_fix) / (fixed * lax.rsqrt(fixed) + tiny_eps) + decay_rate * master


def sums_kernel(tensors, by_tensor, master, new_moment, new_second, weight_line, spread, scaled):
    total = jnp.zeros((tensors, 2 * lanes), f32)
    for start in range(0, by_tensor.shape[1], 2 * lanes):
        part = slice(start, start + 2 * lanes)
        update_dir = direction(new_moment[part, :], new_second[part, :], master[part, :])
        scaled[part, :] = learn_rate * update_dir
        total = total + jnp.dot(
            by_tensor[:, part],
            jnp.concatenate(halves(update_dir * update_dir), axis=1),
            preferred_element_type=f32,
        )
    line = weight_line[...] + as_line(total, tensors, tensors)
    spread[...] = jnp.broadcast_to(line[None], spread.shape)


def apply_kernel(tensors, gathered, by_block, scaled, *rest):
    change = rest[-1]
    line = jnp.sum(gathered[...], axis=0)
    trust = jnp.sqrt(line[:, :tensors]) / (jnp.sqrt(line[:, tensors:]) + tiny_eps)
    square = (tensors, tensors)
    here = lax.broadcasted_iota(jnp.int32, square, 1) == lax.broadcasted_iota(jnp.int32, square, 0)
    column = jnp.sum(jnp.where(here, jnp.broadcast_to(trust, square), 0.0), axis=1, keepdims=True)
    parts = list(thirds(jnp.broadcast_to(column, (tensors, lanes))))
    thrice = by_block.shape[1]
    if thrice > 3 * tensors:
        parts.append(jnp.zeros((thrice - 3 * tensors, lanes), bf16))
    parts = jnp.concatenate(parts, axis=0)
    for start in range(0, scaled.shape[0], lanes):
        part = slice(start, start + lanes)
        scale = jnp.dot(by_block[part, :], parts, preferred_element_type=f32)
        change[part, :] = scaled[part, :] * scale


def on_device(gradients, master, moment, second, segment_ids):
    replicas = lax.axis_size("dp")
    devices = replicas * lax.axis_size("shard")
    tensors = devices // 2
    blocks = segment_ids.shape[0]
    thrice = pl.cdiv(3 * tensors, lanes) * lanes
    ids = segment_ids.reshape(1, blocks)
    master, moment, second = (a.reshape(blocks, lanes) for a in (master, moment, second))
    row = jax.ShapeDtypeStruct((blocks, lanes), bf16)
    wide = jax.ShapeDtypeStruct((blocks, lanes), f32)
    step = 128
    far = pl.BlockSpec(memory_space=pltpu.HBM)
    near = pl.BlockSpec(memory_space=pltpu.VMEM)
    layout = (replicas, blocks * lanes)
    scratch = [
        pltpu.VMEM((step * replicas, lanes), f32),
        pltpu.VMEM(layout, bf16),
        pltpu.SemaphoreType.DMA((pieces,)),
    ]

    rows = call(
        functools.partial(split_kernel, step), [row] * replicas, [pltpu.VMEM((replicas, step * lanes), f32)]
    )(gradients[0])
    received = {
        k: lax.ppermute(rows[k], "dp", [(i, i ^ k) for i in range(replicas)])
        for k in reversed(range(1, replicas))
    }
    old_moment, old_second, by_tensor, by_block, weight_line = call(
        functools.partial(prepare_kernel, tensors),
        [
            wide,
            wide,
            jax.ShapeDtypeStruct((tensors, blocks), bf16),
            jax.ShapeDtypeStruct((blocks, thrice), bf16),
            jax.ShapeDtypeStruct((1, 2 * tensors), f32),
        ],
    )(ids, master, moment, second)
    summed = rows[0].astype(f32)
    for k in range(1, replicas):
        summed = summed + received[k].astype(f32)
    grad = summed / replicas
    new_moment = old_moment + 0.1 * grad
    new_second = old_second + 0.001 * grad * grad
    spread, scaled = call(
        functools.partial(sums_kernel, tensors),
        [jax.ShapeDtypeStruct((devices, 1, 2 * tensors), f32), wide],
    )(by_tensor, master, new_moment, new_second, weight_line)
    gathered = lax.all_to_all(spread, both, 0, 0, tiled=True)
    change = call(functools.partial(apply_kernel, tensors), wide)(
        gathered, by_block, scaled, new_moment, new_second
    )
    new_master = master - change
    whole = lax.all_gather(new_master.astype(bf16), "dp", axis=0, tiled=True)
    scratch[0] = pltpu.VMEM((replicas, step * lanes), f32)
    weights = call(
        functools.partial(join_kernel, step),
        jax.ShapeDtypeStruct(layout, bf16),
        scratch,
        in_specs=[near, near],
        out_specs=far,
    )(whole, new_master)
    return (weights, new_master.reshape(-1), new_moment.reshape(-1), new_second.reshape(-1))


def solution(mesh):
    placed = (
        P("dp", None, "shard"),
        P(("dp", "shard")),
        P(("dp", "shard")),
        P(("dp", "shard")),
        P(("dp", "shard")),
    )
    return jax.shard_map(
        on_device,
        mesh=mesh,
        in_specs=placed,
        out_specs=(P(None, "shard"), P(("dp", "shard")), P(("dp", "shard")), P(("dp", "shard"))),
        check_vma=False,
    )
```

```python
import functools

import jax
import jax.numpy as jnp
from jax import lax
from jax.experimental import pallas as pl
from jax.experimental.pallas import tpu as pltpu
from jax.sharding import PartitionSpec as P

first_fix = 1.0 - 0.9**20
second_fix = 1.0 - 0.999**20
learn_rate = 0.2
decay_rate = 0.01
tiny_eps = 1e-06
both = ("dp", "shard")
lanes = 128
pieces = 6
f32, bf16 = jnp.float32, jnp.bfloat16
grant = 8 << 20
most = 55343328
more = 55043328
loads = 12


def call(kernel, outs, scratch=(), work=1 << 20, limit=grant, **specs):
    return pl.pallas_call(
        kernel,
        out_shape=outs,
        scratch_shapes=list(scratch),
        compiler_params=pltpu.CompilerParams(vmem_limit_bytes=limit),
        cost_estimate=pl.CostEstimate(flops=work, bytes_accessed=work, transcendentals=0),
        **specs,
    )


def halves(value):
    high = value.astype(bf16)
    return high, (value - high.astype(f32)).astype(bf16)


def thirds(value):
    high, rest = value.astype(bf16), value
    rest = value - high.astype(f32)
    middle = rest.astype(bf16)
    return high, middle, (rest - middle.astype(f32)).astype(bf16)


def split_kernel(step, gradients, *rest):
    rows, (room, buffer, sems) = rest[:-3], rest[-3:]
    count = len(rows)
    mine = lax.axis_index("dp")
    width = gradients.shape[1] // loads
    copies = [
        pltpu.make_async_copy(
            gradients.at[:, pl.ds(p * width, width)], buffer.at[:, pl.ds(p * width, width)], sems.at[p]
        )
        for p in range(loads)
    ]
    for copy in copies:
        copy.start()

    def body(j, _):
        part = pl.ds(pl.multiple_of(j * step, step), step)
        columns = pl.ds(pl.multiple_of(j * step * lanes, lanes), step * lanes)
        room[...] = buffer[:, columns].astype(f32)
        for k in range(count):
            rows[k][part, :] = room[pl.ds(mine ^ k, 1), :].reshape(step, lanes).astype(bf16)
        return 0

    turns = width // lanes // step
    for p, copy in enumerate(copies):
        copy.wait()
        lax.fori_loop(p * turns, (p + 1) * turns, body, 0)


def join_kernel(step, rows, new_master, weights, room, buffer, sems):
    count = weights.shape[0]
    blocks = rows.shape[0] // count
    width = weights.shape[1] // pieces
    copies = [
        pltpu.make_async_copy(
            buffer.at[:, pl.ds(p * width, width)], weights.at[:, pl.ds(p * width, width)], sems.at[p]
        )
        for p in range(pieces)
    ]

    def body(j, _):
        for k in range(count):
            room[k : k + 1, :] = (
                rows[pl.ds(pl.multiple_of(k * blocks + j * step, step), step), :]
                .astype(f32)
                .reshape(1, step * lanes)
            )
        start = pl.multiple_of(j * step * lanes, lanes)
        buffer[:, pl.ds(start, step * lanes)] = room[...].astype(bf16)
        return 0

    turns = width // lanes // step
    for p, copy in enumerate(copies):
        lax.fori_loop(p * turns, (p + 1) * turns, body, 0)
        copy.start()
    for copy in copies:
        copy.wait()


def prepare_kernel(tensors, ids, *rest):
    far, (master, old_moment, old_second, by_tensor, by_block, sums), rest = rest[:3], rest[3:9], rest[9:]
    moment, second, sems = rest
    copies = [
        pltpu.make_async_copy(source, target, sems.at[i])
        for i, (source, target) in enumerate(zip(far, (master, moment, second)))
    ]
    for copy in copies:
        copy.start()
    blocks = ids.shape[1]
    thrice = by_block.shape[1]
    for start in range(0, blocks, lanes):
        part = slice(start, start + lanes)
        tensor = lax.broadcasted_iota(jnp.int32, (thrice, lanes), 0)
        wrapped = sum(
            jnp.where((tensor >= k * tensors) & (tensor < (k + 1) * tensors), tensor - k * tensors, 0)
            for k in range(3)
        )
        inside = tensor < 3 * tensors
        hot = jnp.where(inside & (ids[:, part] == wrapped), 1.0, 0.0)
        by_tensor[:, part] = hot[:tensors].astype(bf16)
        for at in range(0, thrice, lanes):
            by_block[part, at : at + lanes] = hot[at : at + lanes].T.astype(bf16)
    for copy in copies:
        copy.wait()
    total = jnp.zeros((tensors, 2 * lanes), f32)
    for start in range(0, blocks, lanes):
        part = slice(start, start + lanes)
        old_moment[part, :] = 0.9 * moment[part, :]
        old_second[part, :] = 0.999 * second[part, :]
        old = master[part, :]
        total = total + jnp.dot(
            by_tensor[:, part],
            jnp.concatenate(halves(old * old), axis=1),
            preferred_element_type=f32,
        )
    sums[...] = as_line(total, tensors, 0)


def as_line(total, tensors, first):
    column = jnp.sum(total[:, :lanes] + total[:, lanes:], axis=1, keepdims=True)
    shape = (tensors, 2 * tensors)
    here = (
        lax.broadcasted_iota(jnp.int32, shape, 1) == lax.broadcasted_iota(jnp.int32, shape, 0) + first
    )
    return jnp.sum(jnp.where(here, jnp.broadcast_to(column, shape), 0.0), axis=0, keepdims=True)


def direction(new_moment, new_second, master):
    fixed = new_second * (1.0 / second_fix)
    return new_moment * (1.0 / first_fix) / (fixed * lax.rsqrt(fixed) + tiny_eps) + decay_rate * master


def sums_kernel(tensors, by_tensor, master, new_moment, new_second, weight_line, spread, scaled):
    total = jnp.zeros((tensors, 2 * lanes), f32)
    for start in range(0, by_tensor.shape[1], 2 * lanes):
        part = slice(start, start + 2 * lanes)
        update_dir = direction(new_moment[part, :], new_second[part, :], master[part, :])
        scaled[part, :] = learn_rate * update_dir
        total = total + jnp.dot(
            by_tensor[:, part],
            jnp.concatenate(halves(update_dir * update_dir), axis=1),
            preferred_element_type=f32,
        )
    line = weight_line[...] + as_line(total, tensors, tensors)
    spread[...] = jnp.broadcast_to(line[None], spread.shape)


def apply_kernel(tensors, gathered, by_block, scaled, *rest):
    change = rest[-1]
    line = jnp.sum(gathered[...], axis=0)
    trust = jnp.sqrt(line[:, :tensors]) / (jnp.sqrt(line[:, tensors:]) + tiny_eps)
    square = (tensors, tensors)
    here = lax.broadcasted_iota(jnp.int32, square, 1) == lax.broadcasted_iota(jnp.int32, square, 0)
    column = jnp.sum(jnp.where(here, jnp.broadcast_to(trust, square), 0.0), axis=1, keepdims=True)
    parts = list(thirds(jnp.broadcast_to(column, (tensors, lanes))))
    thrice = by_block.shape[1]
    if thrice > 3 * tensors:
        parts.append(jnp.zeros((thrice - 3 * tensors, lanes), bf16))
    parts = jnp.concatenate(parts, axis=0)
    for start in range(0, scaled.shape[0], lanes):
        part = slice(start, start + lanes)
        scale = jnp.dot(by_block[part, :], parts, preferred_element_type=f32)
        change[part, :] = scaled[part, :] * scale


def on_device(gradients, master, moment, second, segment_ids):
    replicas = lax.axis_size("dp")
    devices = replicas * lax.axis_size("shard")
    tensors = devices // 2
    blocks = segment_ids.shape[0]
    thrice = pl.cdiv(3 * tensors, lanes) * lanes
    ids = segment_ids.reshape(1, blocks)
    master, moment, second = (a.reshape(blocks, lanes) for a in (master, moment, second))
    row = jax.ShapeDtypeStruct((blocks, lanes), bf16)
    wide = jax.ShapeDtypeStruct((blocks, lanes), f32)
    step = 128
    far = pl.BlockSpec(memory_space=pltpu.HBM)
    near = pl.BlockSpec(memory_space=pltpu.VMEM)
    layout = (replicas, blocks * lanes)
    scratch = [
        pltpu.VMEM((step * replicas, lanes), f32),
        pltpu.VMEM(layout, bf16),
        pltpu.SemaphoreType.DMA((pieces,)),
    ]

    rows = call(
        functools.partial(split_kernel, blocks // loads),
        [row] * replicas,
        [
            pltpu.VMEM((replicas, blocks // loads * lanes), f32),
            pltpu.VMEM(layout, bf16),
            pltpu.SemaphoreType.DMA((loads,)),
        ],
        in_specs=[far],
        limit=most,
    )(gradients[0])
    received = {
        k: lax.ppermute(rows[k], "dp", [(i, i ^ k) for i in range(replicas)])
        for k in reversed(range(1, replicas))
    }
    master, old_moment, old_second, by_tensor, by_block, weight_line = call(
        functools.partial(prepare_kernel, tensors),
        [
            wide,
            wide,
            wide,
            jax.ShapeDtypeStruct((tensors, blocks), bf16),
            jax.ShapeDtypeStruct((blocks, thrice), bf16),
            jax.ShapeDtypeStruct((1, 2 * tensors), f32),
        ],
        [pltpu.VMEM(wide.shape, f32), pltpu.VMEM(wide.shape, f32), pltpu.SemaphoreType.DMA((3,))],
        in_specs=[near, far, far, far],
        limit=more,
    )(ids, master, moment, second)
    summed = rows[0].astype(f32)
    for k in range(1, replicas):
        summed = summed + received[k].astype(f32)
    grad = summed / replicas
    new_moment = old_moment + 0.1 * grad
    new_second = old_second + 0.001 * grad * grad
    spread, scaled = call(
        functools.partial(sums_kernel, tensors),
        [jax.ShapeDtypeStruct((devices, 1, 2 * tensors), f32), wide],
    )(by_tensor, master, new_moment, new_second, weight_line)
    gathered = lax.all_to_all(spread, both, 0, 0, tiled=True)
    change = call(functools.partial(apply_kernel, tensors), wide)(
        gathered, by_block, scaled, new_moment, new_second
    )
    new_master = master - change
    whole = lax.all_gather(new_master.astype(bf16), "dp", axis=0, tiled=True)
    scratch[0] = pltpu.VMEM((replicas, step * lanes), f32)
    weights = call(
        functools.partial(join_kernel, step),
        jax.ShapeDtypeStruct(layout, bf16),
        scratch,
        in_specs=[near, near],
        out_specs=far,
    )(whole, new_master)
    return (weights, new_master.reshape(-1), new_moment.reshape(-1), new_second.reshape(-1))


def solution(mesh):
    placed = (
        P("dp", None, "shard"),
        P(("dp", "shard")),
        P(("dp", "shard")),
        P(("dp", "shard")),
        P(("dp", "shard")),
    )
    return jax.shard_map(
        on_device,
        mesh=mesh,
        in_specs=placed,
        out_specs=(P(None, "shard"), P(("dp", "shard")), P(("dp", "shard")), P(("dp", "shard"))),
        check_vma=False,
    )
```

```python
import functools

import jax
import jax.numpy as jnp
from jax import lax
from jax.experimental import pallas as pl
from jax.experimental.pallas import tpu as pltpu
from jax.sharding import PartitionSpec as P

first_fix = 1.0 - 0.9**20
second_fix = 1.0 - 0.999**20
learn_rate = 0.2
decay_rate = 0.01
tiny_eps = 1e-06
both = ("dp", "shard")
lanes = 128
pieces = 6
f32, bf16 = jnp.float32, jnp.bfloat16
grant = 8 << 20
most = 55343328
more = 55043328
loads = 12


def call(kernel, outs, scratch=(), work=1 << 20, limit=grant, **specs):
    return pl.pallas_call(
        kernel,
        out_shape=outs,
        scratch_shapes=list(scratch),
        compiler_params=pltpu.CompilerParams(vmem_limit_bytes=limit),
        cost_estimate=pl.CostEstimate(flops=work, bytes_accessed=work, transcendentals=0),
        **specs,
    )


def halves(value):
    high = value.astype(bf16)
    return high, (value - high.astype(f32)).astype(bf16)


def thirds(value):
    high, rest = value.astype(bf16), value
    rest = value - high.astype(f32)
    middle = rest.astype(bf16)
    return high, middle, (rest - middle.astype(f32)).astype(bf16)


def split_kernel(step, gradients, *rest):
    rows, (room, buffer, sems) = rest[:-3], rest[-3:]
    count = len(rows)
    mine = lax.axis_index("dp")
    width = gradients.shape[1] // loads
    copies = [
        pltpu.make_async_copy(
            gradients.at[:, pl.ds(p * width, width)], buffer.at[:, pl.ds(p * width, width)], sems.at[p]
        )
        for p in range(loads)
    ]
    for copy in copies:
        copy.start()

    def body(j, _):
        part = pl.ds(pl.multiple_of(j * step, step), step)
        columns = pl.ds(pl.multiple_of(j * step * lanes, lanes), step * lanes)
        room[...] = buffer[:, columns].astype(f32)
        for k in range(count):
            rows[k][part, :] = room[pl.ds(mine ^ k, 1), :].reshape(step, lanes).astype(bf16)
        return 0

    turns = width // lanes // step
    for p, copy in enumerate(copies):
        copy.wait()
        lax.fori_loop(p * turns, (p + 1) * turns, body, 0)


def join_kernel(step, rows, new_master, weights, room, buffer, sems):
    count = weights.shape[0]
    blocks = rows.shape[0] // count
    width = weights.shape[1] // pieces
    copies = [
        pltpu.make_async_copy(
            buffer.at[:, pl.ds(p * width, width)], weights.at[:, pl.ds(p * width, width)], sems.at[p]
        )
        for p in range(pieces)
    ]

    def body(j, _):
        for k in range(count):
            room[k : k + 1, :] = (
                rows[pl.ds(pl.multiple_of(k * blocks + j * step, step), step), :]
                .astype(f32)
                .reshape(1, step * lanes)
            )
        start = pl.multiple_of(j * step * lanes, lanes)
        buffer[:, pl.ds(start, step * lanes)] = room[...].astype(bf16)
        return 0

    turns = width // lanes // step
    for p, copy in enumerate(copies):
        lax.fori_loop(p * turns, (p + 1) * turns, body, 0)
        copy.start()
    for copy in copies:
        copy.wait()


def prepare_kernel(tensors, ids, *rest):
    far, (master, old_moment, old_second, by_tensor, by_block, sums), rest = rest[:3], rest[3:9], rest[9:]
    moment, second, sems = rest
    copies = [
        pltpu.make_async_copy(source, target, sems.at[i])
        for i, (source, target) in enumerate(zip(far, (master, moment, second)))
    ]
    for copy in copies:
        copy.start()
    blocks = ids.shape[1]
    thrice = by_block.shape[1]
    for start in range(0, blocks, lanes):
        part = slice(start, start + lanes)
        tensor = lax.broadcasted_iota(jnp.int32, (thrice, lanes), 0)
        wrapped = sum(
            jnp.where((tensor >= k * tensors) & (tensor < (k + 1) * tensors), tensor - k * tensors, 0)
            for k in range(3)
        )
        inside = tensor < 3 * tensors
        hot = jnp.where(inside & (ids[:, part] == wrapped), 1.0, 0.0)
        by_tensor[:, part] = hot[:tensors].astype(bf16)
        for at in range(0, thrice, lanes):
            by_block[part, at : at + lanes] = hot[at : at + lanes].T.astype(bf16)
    for copy in copies:
        copy.wait()
    total = jnp.zeros((tensors, 2 * lanes), f32)
    for start in range(0, blocks, lanes):
        part = slice(start, start + lanes)
        old_moment[part, :] = 0.9 * moment[part, :]
        old_second[part, :] = 0.999 * second[part, :]
        old = master[part, :]
        total = total + jnp.dot(
            by_tensor[:, part],
            jnp.concatenate(halves(old * old), axis=1),
            preferred_element_type=f32,
        )
    sums[...] = as_line(total, tensors, 0)


def early_kernel(*refs):
    *rows, total = refs
    summed = rows[0][...].astype(f32)
    for row in rows[1:]:
        summed = summed + row[...].astype(f32)
    total[...] = summed


def as_line(total, tensors, first):
    column = jnp.sum(total[:, :lanes] + total[:, lanes:], axis=1, keepdims=True)
    shape = (tensors, 2 * tensors)
    here = (
        lax.broadcasted_iota(jnp.int32, shape, 1) == lax.broadcasted_iota(jnp.int32, shape, 0) + first
    )
    return jnp.sum(jnp.where(here, jnp.broadcast_to(column, shape), 0.0), axis=0, keepdims=True)


def direction(new_moment, new_second, master):
    fixed = new_second * (1.0 / second_fix)
    return new_moment * (1.0 / first_fix) / (fixed * lax.rsqrt(fixed) + tiny_eps) + decay_rate * master


def sums_kernel(tensors, by_tensor, master, new_moment, new_second, weight_line, spread, scaled):
    total = jnp.zeros((tensors, 2 * lanes), f32)
    for start in range(0, by_tensor.shape[1], 2 * lanes):
        part = slice(start, start + 2 * lanes)
        update_dir = direction(new_moment[part, :], new_second[part, :], master[part, :])
        scaled[part, :] = learn_rate * update_dir
        total = total + jnp.dot(
            by_tensor[:, part],
            jnp.concatenate(halves(update_dir * update_dir), axis=1),
            preferred_element_type=f32,
        )
    line = weight_line[...] + as_line(total, tensors, tensors)
    spread[...] = jnp.broadcast_to(line[None], spread.shape)


def apply_kernel(tensors, gathered, by_block, scaled, *rest):
    change = rest[-1]
    line = jnp.sum(gathered[...], axis=0)
    trust = jnp.sqrt(line[:, :tensors]) / (jnp.sqrt(line[:, tensors:]) + tiny_eps)
    square = (tensors, tensors)
    here = lax.broadcasted_iota(jnp.int32, square, 1) == lax.broadcasted_iota(jnp.int32, square, 0)
    column = jnp.sum(jnp.where(here, jnp.broadcast_to(trust, square), 0.0), axis=1, keepdims=True)
    parts = list(thirds(jnp.broadcast_to(column, (tensors, lanes))))
    thrice = by_block.shape[1]
    if thrice > 3 * tensors:
        parts.append(jnp.zeros((thrice - 3 * tensors, lanes), bf16))
    parts = jnp.concatenate(parts, axis=0)
    for start in range(0, scaled.shape[0], lanes):
        part = slice(start, start + lanes)
        scale = jnp.dot(by_block[part, :], parts, preferred_element_type=f32)
        change[part, :] = scaled[part, :] * scale


def on_device(gradients, master, moment, second, segment_ids):
    replicas = lax.axis_size("dp")
    devices = replicas * lax.axis_size("shard")
    tensors = devices // 2
    blocks = segment_ids.shape[0]
    thrice = pl.cdiv(3 * tensors, lanes) * lanes
    ids = segment_ids.reshape(1, blocks)
    master, moment, second = (a.reshape(blocks, lanes) for a in (master, moment, second))
    row = jax.ShapeDtypeStruct((blocks, lanes), bf16)
    wide = jax.ShapeDtypeStruct((blocks, lanes), f32)
    step = 128
    far = pl.BlockSpec(memory_space=pltpu.HBM)
    near = pl.BlockSpec(memory_space=pltpu.VMEM)
    layout = (replicas, blocks * lanes)
    scratch = [
        pltpu.VMEM((step * replicas, lanes), f32),
        pltpu.VMEM(layout, bf16),
        pltpu.SemaphoreType.DMA((pieces,)),
    ]

    rows = call(
        functools.partial(split_kernel, blocks // loads),
        [row] * replicas,
        [
            pltpu.VMEM((replicas, blocks // loads * lanes), f32),
            pltpu.VMEM(layout, bf16),
            pltpu.SemaphoreType.DMA((loads,)),
        ],
        in_specs=[far],
        limit=most,
    )(gradients[0])
    received = {
        k: lax.ppermute(rows[k], "dp", [(i, i ^ k) for i in range(replicas)])
        for k in reversed(range(1, replicas))
    }
    master, old_moment, old_second, by_tensor, by_block, weight_line = call(
        functools.partial(prepare_kernel, tensors),
        [
            wide,
            wide,
            wide,
            jax.ShapeDtypeStruct((tensors, blocks), bf16),
            jax.ShapeDtypeStruct((blocks, thrice), bf16),
            jax.ShapeDtypeStruct((1, 2 * tensors), f32),
        ],
        [pltpu.VMEM(wide.shape, f32), pltpu.VMEM(wide.shape, f32), pltpu.SemaphoreType.DMA((3,))],
        in_specs=[near, far, far, far],
        limit=more,
    )(ids, master, moment, second)
    early = call(early_kernel, wide)(rows[0], *(received[k] for k in range(1, replicas // 2)))
    summed = early
    for k in range(replicas // 2, replicas):
        summed = summed + received[k].astype(f32)
    grad = summed / replicas
    new_moment = old_moment + 0.1 * grad
    new_second = old_second + 0.001 * grad * grad
    spread, scaled = call(
        functools.partial(sums_kernel, tensors),
        [jax.ShapeDtypeStruct((devices, 1, 2 * tensors), f32), wide],
    )(by_tensor, master, new_moment, new_second, weight_line)
    gathered = lax.all_to_all(spread, both, 0, 0, tiled=True)
    change = call(functools.partial(apply_kernel, tensors), wide)(
        gathered, by_block, scaled, new_moment, new_second
    )
    new_master = master - change
    whole = lax.all_gather(new_master.astype(bf16), "dp", axis=0, tiled=True)
    scratch[0] = pltpu.VMEM((replicas, step * lanes), f32)
    weights = call(
        functools.partial(join_kernel, step),
        jax.ShapeDtypeStruct(layout, bf16),
        scratch,
        in_specs=[near, near],
        out_specs=far,
    )(whole, new_master)
    return (weights, new_master.reshape(-1), new_moment.reshape(-1), new_second.reshape(-1))


def solution(mesh):
    placed = (
        P("dp", None, "shard"),
        P(("dp", "shard")),
        P(("dp", "shard")),
        P(("dp", "shard")),
        P(("dp", "shard")),
    )
    return jax.shard_map(
        on_device,
        mesh=mesh,
        in_specs=placed,
        out_specs=(P(None, "shard"), P(("dp", "shard")), P(("dp", "shard")), P(("dp", "shard"))),
        check_vma=False,
    )
```

```python
import functools

import jax
import jax.numpy as jnp
from jax import lax
from jax.experimental import pallas as pl
from jax.experimental.pallas import tpu as pltpu
from jax.sharding import PartitionSpec as P

first_fix = 1.0 - 0.9**20
second_fix = 1.0 - 0.999**20
learn_rate = 0.2
decay_rate = 0.01
tiny_eps = 1e-06
both = ("dp", "shard")
lanes = 128
pieces = 6
f32, bf16 = jnp.float32, jnp.bfloat16
grant = 8 << 20
most = 55343328
more = 55043328
loads = 12


def call(kernel, outs, scratch=(), work=1 << 20, limit=grant, **specs):
    return pl.pallas_call(
        kernel,
        out_shape=outs,
        scratch_shapes=list(scratch),
        compiler_params=pltpu.CompilerParams(vmem_limit_bytes=limit),
        cost_estimate=pl.CostEstimate(flops=work, bytes_accessed=work, transcendentals=0),
        **specs,
    )


def halves(value):
    high = value.astype(bf16)
    return high, (value - high.astype(f32)).astype(bf16)


def thirds(value):
    high, rest = value.astype(bf16), value
    rest = value - high.astype(f32)
    middle = rest.astype(bf16)
    return high, middle, (rest - middle.astype(f32)).astype(bf16)


def split_kernel(step, gradients, *rest):
    rows, (room, buffer, sems) = rest[:-3], rest[-3:]
    count = len(rows)
    mine = lax.axis_index("dp")
    width = gradients.shape[1] // loads
    copies = [
        pltpu.make_async_copy(
            gradients.at[:, pl.ds(p * width, width)], buffer.at[:, pl.ds(p * width, width)], sems.at[p]
        )
        for p in range(loads)
    ]
    for copy in copies:
        copy.start()

    def body(j, _):
        part = pl.ds(pl.multiple_of(j * step, step), step)
        columns = pl.ds(pl.multiple_of(j * step * lanes, lanes), step * lanes)
        room[...] = buffer[:, columns].astype(f32)
        for k in range(count):
            rows[k][part, :] = room[pl.ds(mine ^ k, 1), :].reshape(step, lanes).astype(bf16)
        return 0

    turns = width // lanes // step
    for p, copy in enumerate(copies):
        copy.wait()
        lax.fori_loop(p * turns, (p + 1) * turns, body, 0)


def join_kernel(step, rows, new_master, weights, room, buffer, sems):
    count = weights.shape[0]
    blocks = rows.shape[0] // count
    width = weights.shape[1] // pieces
    copies = [
        pltpu.make_async_copy(
            buffer.at[:, pl.ds(p * width, width)], weights.at[:, pl.ds(p * width, width)], sems.at[p]
        )
        for p in range(pieces)
    ]

    def body(j, _):
        for k in range(count):
            room[k : k + 1, :] = (
                rows[pl.ds(pl.multiple_of(k * blocks + j * step, step), step), :]
                .astype(f32)
                .reshape(1, step * lanes)
            )
        start = pl.multiple_of(j * step * lanes, lanes)
        buffer[:, pl.ds(start, step * lanes)] = room[...].astype(bf16)
        return 0

    turns = width // lanes // step
    for p, copy in enumerate(copies):
        lax.fori_loop(p * turns, (p + 1) * turns, body, 0)
        copy.start()
    for copy in copies:
        copy.wait()


def prepare_kernel(tensors, ids, *rest):
    far, (master, old_moment, old_second, by_tensor, by_block, sums), rest = rest[:3], rest[3:9], rest[9:]
    moment, second, sems = rest
    copies = [
        pltpu.make_async_copy(source, target, sems.at[i])
        for i, (source, target) in enumerate(zip(far, (master, moment, second)))
    ]
    for copy in copies:
        copy.start()
    blocks = ids.shape[1]
    thrice = by_block.shape[1]
    for start in range(0, blocks, lanes):
        part = slice(start, start + lanes)
        tensor = lax.broadcasted_iota(jnp.int32, (thrice, lanes), 0)
        wrapped = sum(
            jnp.where((tensor >= k * tensors) & (tensor < (k + 1) * tensors), tensor - k * tensors, 0)
            for k in range(3)
        )
        inside = tensor < 3 * tensors
        hot = jnp.where(inside & (ids[:, part] == wrapped), 1.0, 0.0)
        by_tensor[:, part] = hot[:tensors].astype(bf16)
        for at in range(0, thrice, lanes):
            by_block[part, at : at + lanes] = hot[at : at + lanes].T.astype(bf16)
    for copy in copies:
        copy.wait()
    total = jnp.zeros((tensors, 2 * lanes), f32)
    for start in range(0, blocks, lanes):
        part = slice(start, start + lanes)
        old_moment[part, :] = 0.9 * moment[part, :]
        old_second[part, :] = 0.999 * second[part, :]
        old = master[part, :]
        total = total + jnp.dot(
            by_tensor[:, part],
            jnp.concatenate(halves(old * old), axis=1),
            preferred_element_type=f32,
        )
    sums[...] = as_line(total, tensors, 0)


def early_kernel(*refs):
    *rows, total = refs
    summed = rows[0][...].astype(f32)
    for row in rows[1:]:
        summed = summed + row[...].astype(f32)
    total[...] = summed


def as_line(total, tensors, first):
    column = jnp.sum(total[:, :lanes] + total[:, lanes:], axis=1, keepdims=True)
    shape = (tensors, 2 * tensors)
    here = (
        lax.broadcasted_iota(jnp.int32, shape, 1) == lax.broadcasted_iota(jnp.int32, shape, 0) + first
    )
    return jnp.sum(jnp.where(here, jnp.broadcast_to(column, shape), 0.0), axis=0, keepdims=True)


def direction(new_moment, new_second, master):
    fixed = new_second * (1.0 / second_fix)
    return new_moment * (1.0 / first_fix) / (fixed * lax.rsqrt(fixed) + tiny_eps) + decay_rate * master


def sums_kernel(tensors, by_tensor, master, new_moment, new_second, weight_line, spread, scaled):
    total = jnp.zeros((tensors, 2 * lanes), f32)
    for start in range(0, by_tensor.shape[1], 3 * lanes):
        part = slice(start, start + 3 * lanes)
        update_dir = direction(new_moment[part, :], new_second[part, :], master[part, :])
        scaled[part, :] = learn_rate * update_dir
        total = total + jnp.dot(
            by_tensor[:, part],
            jnp.concatenate(halves(update_dir * update_dir), axis=1),
            preferred_element_type=f32,
        )
    line = weight_line[...] + as_line(total, tensors, tensors)
    spread[...] = jnp.broadcast_to(line[None], spread.shape)


def apply_kernel(tensors, gathered, by_block, scaled, *rest):
    change = rest[-1]
    line = jnp.sum(gathered[...], axis=0)
    trust = jnp.sqrt(line[:, :tensors]) / (jnp.sqrt(line[:, tensors:]) + tiny_eps)
    square = (tensors, tensors)
    here = lax.broadcasted_iota(jnp.int32, square, 1) == lax.broadcasted_iota(jnp.int32, square, 0)
    column = jnp.sum(jnp.where(here, jnp.broadcast_to(trust, square), 0.0), axis=1, keepdims=True)
    parts = list(thirds(jnp.broadcast_to(column, (tensors, lanes))))
    thrice = by_block.shape[1]
    if thrice > 3 * tensors:
        parts.append(jnp.zeros((thrice - 3 * tensors, lanes), bf16))
    parts = jnp.concatenate(parts, axis=0)
    for start in range(0, scaled.shape[0], lanes):
        part = slice(start, start + lanes)
        scale = jnp.dot(by_block[part, :], parts, preferred_element_type=f32)
        change[part, :] = scaled[part, :] * scale


def on_device(gradients, master, moment, second, segment_ids):
    replicas = lax.axis_size("dp")
    devices = replicas * lax.axis_size("shard")
    tensors = devices // 2
    blocks = segment_ids.shape[0]
    thrice = pl.cdiv(3 * tensors, lanes) * lanes
    ids = segment_ids.reshape(1, blocks)
    master, moment, second = (a.reshape(blocks, lanes) for a in (master, moment, second))
    row = jax.ShapeDtypeStruct((blocks, lanes), bf16)
    wide = jax.ShapeDtypeStruct((blocks, lanes), f32)
    step = 128
    far = pl.BlockSpec(memory_space=pltpu.HBM)
    near = pl.BlockSpec(memory_space=pltpu.VMEM)
    layout = (replicas, blocks * lanes)
    scratch = [
        pltpu.VMEM((step * replicas, lanes), f32),
        pltpu.VMEM(layout, bf16),
        pltpu.SemaphoreType.DMA((pieces,)),
    ]

    rows = call(
        functools.partial(split_kernel, blocks // loads),
        [row] * replicas,
        [
            pltpu.VMEM((replicas, blocks // loads * lanes), f32),
            pltpu.VMEM(layout, bf16),
            pltpu.SemaphoreType.DMA((loads,)),
        ],
        in_specs=[far],
        limit=most,
    )(gradients[0])
    received = {
        k: lax.ppermute(rows[k], "dp", [(i, i ^ k) for i in range(replicas)])
        for k in reversed(range(1, replicas))
    }
    master, old_moment, old_second, by_tensor, by_block, weight_line = call(
        functools.partial(prepare_kernel, tensors),
        [
            wide,
            wide,
            wide,
            jax.ShapeDtypeStruct((tensors, blocks), bf16),
            jax.ShapeDtypeStruct((blocks, thrice), bf16),
            jax.ShapeDtypeStruct((1, 2 * tensors), f32),
        ],
        [pltpu.VMEM(wide.shape, f32), pltpu.VMEM(wide.shape, f32), pltpu.SemaphoreType.DMA((3,))],
        in_specs=[near, far, far, far],
        limit=more,
    )(ids, master, moment, second)
    early = call(early_kernel, wide)(rows[0], *(received[k] for k in range(1, replicas // 2)))
    summed = early
    for k in range(replicas // 2, replicas):
        summed = summed + received[k].astype(f32)
    grad = summed / replicas
    new_moment = old_moment + 0.1 * grad
    new_second = old_second + 0.001 * grad * grad
    spread, scaled = call(
        functools.partial(sums_kernel, tensors),
        [jax.ShapeDtypeStruct((devices, 1, 2 * tensors), f32), wide],
    )(by_tensor, master, new_moment, new_second, weight_line)
    gathered = lax.all_to_all(spread, both, 0, 0, tiled=True)
    change = call(functools.partial(apply_kernel, tensors), wide)(
        gathered, by_block, scaled, new_moment, new_second
    )
    new_master = master - change
    whole = lax.all_gather(new_master.astype(bf16), "dp", axis=0, tiled=True)
    scratch[0] = pltpu.VMEM((replicas, step * lanes), f32)
    weights = call(
        functools.partial(join_kernel, step),
        jax.ShapeDtypeStruct(layout, bf16),
        scratch,
        in_specs=[near, near],
        out_specs=far,
    )(whole, new_master)
    return (weights, new_master.reshape(-1), new_moment.reshape(-1), new_second.reshape(-1))


def solution(mesh):
    placed = (
        P("dp", None, "shard"),
        P(("dp", "shard")),
        P(("dp", "shard")),
        P(("dp", "shard")),
        P(("dp", "shard")),
    )
    return jax.shard_map(
        on_device,
        mesh=mesh,
        in_specs=placed,
        out_specs=(P(None, "shard"), P(("dp", "shard")), P(("dp", "shard")), P(("dp", "shard"))),
        check_vma=False,
    )
```
